16 devices in a mesh: dp: 16 (over z, y, x, core).
Axes of the slice: x: 2, y: 2, z: 2, core: 2. Of those that a mesh axis runs over, the one named last changes fastest.
Arguments:
- img_emb: bfloat16 [24576, 1536], P('dp')
- txt_emb: bfloat16 [24576, 1536], P('dp')
- log_temp: float32 [1], replicated
- logit_bias: float32 [1], replicated
Outputs:
- output 1: float32 [1], replicated
- output 2: float32 [24576, 1536], P('dp')
- output 3: float32 [24576, 1536], P('dp')
- output 4: float32 [1], replicated
- output 5: float32 [1], replicated
All inputs are finite; a program needn't handle non-finite values.
Results may differ from the reference program's by a relative error of at most 0.001.
Values are sent between devices in bfloat16 or wider.
A program may use at most 1 GiB of HBM per device.

```python
import math
import jax
import jax.numpy as jnp
from jax import lax

ROWS = 1536
DEVICES = 16
EMBED = 1536
ROW_BLOCK = 64


def setup_inputs(seed: int = 0) -> dict:
    n_total = ROWS * DEVICES
    sub_keys = jax.random.split(jax.random.key(seed), 6)
    latent = jax.random.normal(sub_keys[0], (n_total, EMBED), jnp.float32)
    shard_shift = jax.random.randint(sub_keys[1], (n_total,), 1, DEVICES)
    partner = (jnp.arange(n_total) + shard_shift * ROWS) % n_total
    img_raw = latent + 0.5 * jax.random.normal(sub_keys[2], (n_total, EMBED), jnp.float32)
    txt_raw = latent + 0.8 * latent[partner] + 0.5 * jax.random.normal(sub_keys[3], (n_total, EMBED), jnp.float32)
    img_emb = img_raw / jnp.linalg.norm(img_raw, axis=1, keepdims=True)
    txt_emb = txt_raw / jnp.linalg.norm(txt_raw, axis=1, keepdims=True)
    log_temp = math.log(2.0 * math.log(n_total)) + jax.random.uniform(sub_keys[4], (1,), jnp.float32, -0.25, 0.25)
    logit_bias = -math.log(n_total) + jax.random.uniform(sub_keys[5], (1,), jnp.float32, -1.0, 1.0)
    return {'img_emb': img_emb.astype(jnp.bfloat16), 'txt_emb': txt_emb.astype(jnp.bfloat16), 'log_temp': log_temp, 'logit_bias': logit_bias}


def reference(img_emb, txt_emb, log_temp, logit_bias):
    n_total = img_emb.shape[0]
    n_blocks = n_total // ROW_BLOCK
    temp_scale = jnp.exp(log_temp[0])
    bias_val = logit_bias[0]
    col_ids = jnp.arange(n_total)
    img_blocks = img_emb.reshape(n_blocks, ROW_BLOCK, EMBED)

    def block_step(loop_state, step_in):
        loss_acc, bias_acc, temp_acc, txt_acc = loop_state
        block_idx, img_block = step_in
        row_ids = block_idx * ROW_BLOCK + jnp.arange(ROW_BLOCK)
        labels = jnp.where(row_ids[:, None] == col_ids[None, :], 1.0, -1.0)
        dot_vals = jnp.dot(img_block, txt_emb.T, preferred_element_type=jnp.float32)
        margin = labels * (temp_scale * dot_vals + bias_val)
        loss_acc = loss_acc + jnp.sum(jax.nn.softplus(-margin))
        grad_coef = -labels * jax.nn.sigmoid(-margin)
        coef_bf16 = grad_coef.astype(jnp.bfloat16)
        bias_acc = bias_acc + jnp.sum(grad_coef)
        temp_acc = temp_acc + jnp.sum(grad_coef * dot_vals)
        img_part = jnp.dot(coef_bf16, txt_emb, preferred_element_type=jnp.float32)
        txt_acc = txt_acc + jnp.dot(coef_bf16.T, img_block, preferred_element_type=jnp.float32)
        return (loss_acc, bias_acc, temp_acc, txt_acc), img_part

    zero_val = jnp.zeros((), jnp.float32)
    init_state = (zero_val, zero_val, zero_val, jnp.zeros((n_total, EMBED), jnp.float32))
    final_state, img_parts = lax.scan(block_step, init_state, (jnp.arange(n_blocks), img_blocks))
    loss_acc, bias_acc, temp_acc, txt_acc = final_state
    factor = temp_scale / n_total
    total_loss = (loss_acc / n_total).reshape(1)
    img_grad = img_parts.reshape(n_total, EMBED) * factor
    txt_grad = txt_acc * factor
    temp_grad = (temp_acc * factor).reshape(1)
    bias_grad = (bias_acc / n_total).reshape(1)
    return (total_loss, img_grad, txt_grad, temp_grad, bias_grad)
```

```python
import functools
import jax
import jax.numpy as jnp
from jax import lax
from jax.experimental import pallas as pl
from jax.experimental.pallas import tpu as pltpu
from jax.sharding import PartitionSpec as P

LOG2E = 1.4426950408889634
LN2 = 0.6931471805599453
BM = 512
STRIP = 32
CHUNK = 512
LANES = 256


def panel_body(cfg, *refs):
    seg_chunks, seg_acc, pieces, tin_flags, diag, bn = cfg
    refs = list(refs)
    take = lambda n: [refs.pop(0) for _ in range(n)]
    nseg, npc = len(seg_chunks), len(pieces)
    (sc,) = take(1)
    (sin,) = take(1)
    imgs, txts = take(nseg), take(npc)
    tins = take(sum(tin_flags))
    iins = take(sum(seg_acc))
    (sums,) = take(1)
    tos, ios = take(npc), take(nseg)
    T, TO, I, A, S, C, CR, tsem, osem, fsem, isem, asem, wsem = refs
    starts = [sum(seg_chunks[:k]) for k in range(nseg + 1)]
    G = starts[-1]
    Q = sum(pieces)
    D = T.shape[1]
    nth = Q // bn
    offs = [sum(pieces[:k]) for k in range(npc)]
    s2_, b2 = sc[0], sc[1]

    def t_copy(j):
        return pltpu.make_async_copy(txts[j], T.at[pl.ds(offs[j], pieces[j])], tsem.at[j])

    def tin_copy(j, r):
        return pltpu.make_async_copy(r, TO.at[pl.ds(offs[j], pieces[j])], osem.at[j])

    runs = []
    for j in range(npc):
        lo = offs[j]
        while lo < offs[j] + pieces[j]:
            hi = min((lo // bn + 1) * bn, offs[j] + pieces[j])
            runs.append((j, lo, hi - lo))
            lo = hi

    def flush(n):
        for q, (j, lo, size) in enumerate(runs):
            if lo // bn == n:
                flush_copy(q).start()

    def flush_copy(q):
        j, lo, size = runs[q]
        return pltpu.make_async_copy(TO.at[pl.ds(lo, size)], tos[j].at[pl.ds(lo - offs[j], size)], fsem.at[q])

    def when_seg(g, fn):
        for k in range(nseg):
            if nseg == 1:
                fn(k)
            else:
                pl.when((g >= starts[k]) & (g < starts[k + 1]))(functools.partial(fn, k))

    acc_src = []
    q = 0
    for k in range(nseg):
        acc_src.append(iins[q] if seg_acc[k] else None)
        q += seg_acc[k]

    def fetch(g):
        def one(k):
            rows = pl.ds((g - starts[k]) * BM, BM)
            pltpu.make_async_copy(imgs[k].at[rows], I.at[g % 4], isem.at[g % 4]).start()
            if seg_acc[k]:
                pltpu.make_async_copy(acc_src[k].at[rows], A.at[g % 4], asem.at[g % 4]).start()

        when_seg(g, one)

    def wait_img(g):
        pltpu.make_async_copy(imgs[0].at[pl.ds(0, BM)], I.at[g % 4], isem.at[g % 4]).wait()

    def open_acc(g):
        def one(k):
            if seg_acc[k]:
                pltpu.make_async_copy(acc_src[k].at[pl.ds(0, BM)], A.at[g % 4], asem.at[g % 4]).wait()
            else:
                A[g % 4] = jnp.zeros((BM, D), jnp.float32)

        when_seg(g, one)

    def put(g):
        def one(k):
            pltpu.make_async_copy(A.at[g % 4], ios[k].at[pl.ds((g - starts[k]) * BM, BM)], wsem.at[g % 4]).start()

        when_seg(g, one)

    def wait_put(g):
        pltpu.make_async_copy(A.at[g % 4], ios[0].at[pl.ds(0, BM)], wsem.at[g % 4]).wait()

    for j in range(npc):
        t_copy(j).start()
    fetch(jnp.int32(0))
    q = 0
    for j in range(npc):
        if tin_flags[j]:
            tin_copy(j, tins[q]).start()
            q += 1
        else:
            TO[pl.ds(offs[j], pieces[j])] = jnp.zeros((pieces[j], D), jnp.float32)
    sums[...] = sin[...]
    for j in range(npc):
        t_copy(j).wait()

    def tile(n):
        return pl.ds(pl.multiple_of(n * bn, bn), bn)


    def s1(g, n):
        S[...] = lax.dot_general(I[g % 4], T[tile(n), :], (((1,), (1,)), ((), ())), preferred_element_type=jnp.float32)

    def s2_strip(g, n, r0, accs, z):
        rs = pl.ds(r0, STRIP)
        dot = S[rs, :]
        bias = b2
        if z is not None:
            bz = z + b2
            bias = jnp.concatenate([bz] * (STRIP // 8), axis=0)
            bias = jnp.concatenate([bias] * (bn // 128), axis=1)
        v = dot * s2_ + bias
        if diag:
            rows = g * BM + r0 + lax.broadcasted_iota(jnp.int32, (STRIP, bn), 0)
            cols = n * bn + lax.broadcasted_iota(jnp.int32, (STRIP, bn), 1)
            on = rows == cols
            v = jnp.where(on, -v, v)
        w = jnp.minimum(v, 120.0)
        e = jnp.exp2(w)
        r = 1.0 / (1.0 + e)
        c = e * r
        fix = (1.0 - r) - c
        lg = jnp.log2(r) - (v - w)
        if diag:
            c = jnp.where(on, -c, c)
        C[rs, :] = c.astype(jnp.bfloat16)
        for q, val in enumerate((lg, fix, c, c * dot)):
            for k in range(0, STRIP, 8):
                for d0 in range(0, bn, LANES):
                    accs[q] = accs[q] + val[k : k + 8, d0 : d0 + LANES]

    def s2(g, n, toks=None):
        accs = [jnp.zeros((8, LANES), jnp.float32)] * 4
        NS = BM // STRIP
        for i in range(NS):
            z = None
            if toks:
                z = toks[min(len(toks) - 1, i * len(toks) // NS)] * 0.0
            s2_strip(g, n, i * STRIP, accs, z)
        for q in range(4):
            sums[q] += accs[q]

    def s3(g, n, toks):
        for d0 in range(0, D, CHUNK):
            val = A[g % 4, :, pl.ds(d0, CHUNK)] + jnp.dot(CR[...], T[tile(n), pl.ds(d0, CHUNK)], preferred_element_type=jnp.float32)
            A[g % 4, :, pl.ds(d0, CHUNK)] = val
            toks.append(val[:8, :128])
        for d0 in range(0, D, CHUNK):
            val = TO[tile(n), pl.ds(d0, CHUNK)] + lax.dot_general(CR[...], I[g % 4, :, pl.ds(d0, CHUNK)], (((0,), (0,)), ((), ())), preferred_element_type=jnp.float32)
            TO[tile(n), pl.ds(d0, CHUNK)] = val
            toks.append(val[:8, :128])

    wait_img(jnp.int32(0))
    if G > 1:
        fetch(jnp.int32(1))
    s1(jnp.int32(0), 0)
    q = 0
    for j in range(npc):
        if tin_flags[j]:
            tin_copy(j, tins[q]).wait()
            q += 1

    def split(t):
        return t // nth, t % nth

    def unit(t, with3):
        g, h = split(t)
        gp, hp = split(t - 1)
        gq, hq = split(t - 2)

        @pl.when(h == 0)
        def _():
            wait_img(g)

            @pl.when(g >= 3)
            def _():
                wait_put(g - 3)

            @pl.when(g + 1 < G)
            def _():
                fetch(g + 1)

        if with3:
            @pl.when(hq == 0)
            def _():
                open_acc(gq)

        toks = []
        if with3:
            CR[...] = C[...]
            s3(gq, hq, toks)
        s2(gp, hp, toks)
        s1(g, h)
        if with3:
            @pl.when(hq == nth - 1)
            def _():
                put(gq)

    unit(jnp.int32(1), False)

    def body(t, carry):
        unit(t, True)
        return carry

    NU = G * nth
    lax.fori_loop(2, NU, body, 0)
    gl = jnp.int32(G - 1)
    ga, ha = (NU - 2) // nth, (NU - 2) % nth
    if ha == 0:
        open_acc(jnp.int32(ga))
    for n in range(nth - 2):
        flush(n)
    CR[...] = C[...]
    toks = []
    s3(jnp.int32(ga), ha, toks)
    s2(gl, nth - 1, toks)
    if ha == nth - 1:
        put(jnp.int32(ga))
    else:
        flush(nth - 2)
    if nth == 1:
        open_acc(gl)
    CR[...] = C[...]
    s3(gl, nth - 1, [])
    put(gl)
    flush(nth - 1)
    for g in range(max(0, G - 3), G):
        wait_put(jnp.int32(g))
    for q in range(len(runs)):
        flush_copy(q).wait()


def panel(sc, sums, imgs, iins, txts, tins, diag=False, bn=512):
    return panel_call(sc, sums, imgs, iins, txts, tins, diag, bn)


def panel_call(sc, sums, imgs, iins, txts, tins, diag, bn):
    D = imgs[0].shape[1]
    cfg = (tuple(a.shape[0] // BM for a in imgs), tuple(a is not None for a in iins), tuple(a.shape[0] for a in txts), tuple(a is not None for a in tins), diag, bn)
    M, Q = sum(a.shape[0] for a in imgs), sum(a.shape[0] for a in txts)
    hbm = pl.BlockSpec(memory_space=pl.ANY)
    args = [sc, sums, *imgs, *txts, *[a for a in tins if a is not None]]
    na = len(args)
    ia = [a for a in iins if a is not None]
    args += ia
    out_shape = [jax.ShapeDtypeStruct(sums.shape, jnp.float32)]
    out_shape += [jax.ShapeDtypeStruct(a.shape, jnp.float32) for a in txts] + [jax.ShapeDtypeStruct(a.shape, jnp.float32) for a in imgs]
    alias = {}
    q = na
    for k, a in enumerate(iins):
        if a is not None:
            alias[q] = 1 + len(txts) + k
            q += 1
    in_specs = [pl.BlockSpec(memory_space=pltpu.SMEM), pl.BlockSpec(memory_space=pltpu.VMEM)] + [hbm] * (len(args) - 2)
    out_specs = [pl.BlockSpec(memory_space=pltpu.VMEM)] + [hbm] * (len(out_shape) - 1)
    outs = pl.pallas_call(
        functools.partial(panel_body, cfg),
        out_shape=out_shape,
        in_specs=in_specs,
        out_specs=out_specs,
        input_output_aliases=alias,
        scratch_shapes=[
            pltpu.VMEM((Q, D), jnp.bfloat16),
            pltpu.VMEM((Q, D), jnp.float32),
            pltpu.VMEM((4, BM, D), jnp.bfloat16),
            pltpu.VMEM((4, BM, D), jnp.float32),
            pltpu.VMEM((BM, bn), jnp.float32),
            pltpu.VMEM((BM, bn), jnp.bfloat16),
            pltpu.VMEM((BM, bn), jnp.bfloat16),
            pltpu.SemaphoreType.DMA((len(txts),)),
            pltpu.SemaphoreType.DMA((len(txts),)),
            pltpu.SemaphoreType.DMA((Q // bn + len(txts),)),
            pltpu.SemaphoreType.DMA((4,)),
            pltpu.SemaphoreType.DMA((4,)),
            pltpu.SemaphoreType.DMA((4,)),
        ],
        cost_estimate=pl.CostEstimate(flops=6 * M * Q * D, bytes_accessed=10 * M * D, transcendentals=3 * M * Q),
        compiler_params=pltpu.CompilerParams(vmem_limit_bytes=58 * 1024 * 1024),
        name="panel",
    )(*args)
    return outs[0], list(outs[1 : 1 + len(txts)]), list(outs[1 + len(txts) :])


def combine_body(starts, factor, base, *refs):
    refs = list(refs)
    out = refs.pop()
    g = pl.program_id(0)
    out[...] = base[...]
    for ref, (lo, hi) in zip(refs, starts):
        @pl.when((g >= lo) & (g < hi))
        def _():
            out[...] += ref[...]

    out[...] *= factor[0]


def combine_call(factor, base, groups):
    rows, D = base.shape
    br = 256
    starts, specs, args = [], [], []
    for group in groups:
        lo = 0
        for piece in group:
            n = piece.shape[0] // br
            starts.append((lo, lo + n))
            specs.append(pl.BlockSpec((br, D), functools.partial(lambda lo, n, g: (jnp.clip(g - lo, 0, n - 1), 0), lo, n)))
            args.append(piece)
            lo += n
    row = pl.BlockSpec((br, D), lambda g: (g, 0))
    return pl.pallas_call(
        functools.partial(combine_body, tuple(starts)),
        grid=(rows // br,),
        out_shape=jax.ShapeDtypeStruct(base.shape, jnp.float32),
        in_specs=[pl.BlockSpec(memory_space=pltpu.SMEM), row, *specs],
        out_specs=row,
        compiler_params=pltpu.CompilerParams(vmem_limit_bytes=32 * 1024 * 1024),
        cost_estimate=pl.CostEstimate(flops=rows * D * 64, bytes_accessed=16 * rows * D, transcendentals=0),
        name="combine",
    )(factor.reshape(1), base, *args)


def add_tail_body(factor, base, piece, out):
    out[...] = base[...] + piece[...] * factor[0]


def add_tail(factor, base, piece):
    rows, D = base.shape
    br = 256
    n = piece.shape[0] // br
    lo = rows // br - n
    late = pl.BlockSpec((br, D), lambda g: (lo + g, 0))
    return pl.pallas_call(
        add_tail_body,
        grid=(n,),
        out_shape=jax.ShapeDtypeStruct(base.shape, jnp.float32),
        in_specs=[pl.BlockSpec(memory_space=pltpu.SMEM), late, pl.BlockSpec((br, D), lambda g: (g, 0))],
        out_specs=late,
        input_output_aliases={1: 0},
        compiler_params=pltpu.CompilerParams(vmem_limit_bytes=32 * 1024 * 1024),
        name="add_tail",
    )(factor.reshape(1), base, piece)


def solution(mesh):
    axis = mesh.axis_names[0]
    n_dev = mesh.shape[axis]

    def swap(a, mask):
        return lax.ppermute(a, axis, [(i, i ^ mask) for i in range(n_dev)])

    CORE, X, Y, Z = 1, 2, 4, 8

    def step(img, txt, log_temp, logit_bias):
        rows = img.shape[0]
        n_total = rows * n_dev
        scale = jnp.exp(log_temp[0])
        sc = jnp.stack([scale * LOG2E, logit_bias[0] * LOG2E])
        sums = jnp.zeros((4, 8, LANES), jnp.float32)
        ha, hb = slice(0, rows // 2), slice(rows // 2, rows)
        x_cut = rows * 2 // 3

        img_c = swap(img, CORE)
        x0 = swap(img[:x_cut], X)
        x1 = swap(img[x_cut:], X)
        xc0 = swap(x0, CORE)
        xc1 = swap(x1, CORE)
        ya = swap(txt[ha], Y)
        zb = swap(txt[hb], Z)
        yza = swap(ya, Z)
        yzb = swap(zb, Y)
        yb = swap(txt[hb], Y)
        za = swap(txt[ha], Z)

        OC, X0, X1 = [img, img_c], [x0, xc0], [x1, xc1]
        N2 = [None, None]

        sums, own, oc = panel(sc, sums, OC, N2, [txt], [None], diag=True)
        sums, own, ax0 = panel(sc, sums, X0, N2, [txt], own)
        sums, p_yz, accs = panel(sc, sums, OC + X0 + X1, oc + ax0 + N2, [yza, yzb], N2)
        ry, rz = swap(p_yz[0], Z), swap(p_yz[1], Y)
        sums, p_zayb, accs = panel(sc, sums, OC + X0 + X1, accs, [za, yb], N2)
        oc, ax0, ax1 = accs[0:2], accs[2:4], accs[4:6]
        fz, fy = swap(p_zayb[0], Z), swap(p_zayb[1], Y)
        sums, p_yazb, ax0 = panel(sc, sums, X0, ax0, [ya, zb], [ry, rz])
        gx0 = swap(ax0[0] + swap(ax0[1], CORE), X)
        sums, p_yazb, accs = panel(sc, sums, OC + X1, oc + ax1, [ya, zb], p_yazb)
        oc, ax1 = accs[0:2], accs[2:4]
        gy, gz = swap(p_yazb[0], Y), swap(p_yazb[1], Z)
        gc = swap(oc[1], CORE)
        sums, own, ax1 = panel(sc, sums, X1, ax1, [txt], own)
        gx1 = swap(ax1[0] + swap(ax1[1], CORE), X)

        factor = scale / n_total
        txt_pre = combine_call(jnp.ones((), jnp.float32), own[0], [[fz, fy]])
        img_pre = combine_call(factor, oc[0], [[gc], [gx0]])
        txt_grad = combine_call(factor, txt_pre, [[gy, gz]])
        img_grad = add_tail(factor, img_pre, gx1)
        tot = jnp.sum(sums, axis=(1, 2))
        for mask in (CORE, Y, Z, X):
            tot = tot + swap(tot, mask)
        loss = -(tot[0:1] * LN2 + tot[1:2]) / n_total
        return loss, img_grad, txt_grad, tot[3:4] * factor, tot[2:3] / n_total

    split = P(axis, None)
    return jax.shard_map(step, mesh=mesh, in_specs=(split, split, P(None), P(None)), out_specs=(P(None), split, split, P(None), P(None)), check_vma=False)
```

```python
import functools
import jax
import jax.numpy as jnp
from jax import lax
from jax.experimental import pallas as pl
from jax.experimental.pallas import tpu as pltpu
from jax.sharding import PartitionSpec as P

LOG2E = 1.4426950408889634
LN2 = 0.6931471805599453
BM = 512
STRIP = 32
CHUNK = 512
LANES = 256


def panel_body(cfg, *refs):
    seg_chunks, seg_acc, pieces, tin_flags, diag, bn, cuts = cfg
    refs = list(refs)
    take = lambda n: [refs.pop(0) for _ in range(n)]
    nseg, npc = len(seg_chunks), len(pieces)
    (sc,) = take(1)
    (sin,) = take(1)
    imgs, txts = take(nseg), take(npc)
    tins = take(sum(tin_flags))
    iins = take(sum(seg_acc))
    (sums,) = take(1)
    tos, ios = take(len(cuts)), take(nseg)
    T, TO, I, A, S, C, CR, tsem, osem, fsem, isem, asem, wsem = refs
    starts = [sum(seg_chunks[:k]) for k in range(nseg + 1)]
    G = starts[-1]
    Q = sum(pieces)
    D = T.shape[1]
    nth = Q // bn
    s2_, b2 = sc[0], sc[1]

    def cut_runs(sizes):
        runs, at = [], 0
        for j, size in enumerate(sizes):
            lo = at
            while lo < at + size:
                hi = min((lo // bn + 1) * bn, at + size)
                runs.append((j, lo, hi - lo, lo - at))
                lo = hi
            at += size
        return runs

    runs, out_runs = cut_runs(pieces), cut_runs(cuts)

    def load_text(n):
        for j, lo, size, at in runs:
            if lo // bn == n:
                pltpu.make_async_copy(txts[j].at[pl.ds(at, size)], T.at[pl.ds(lo, size)], tsem.at[n]).start()

    def wait_text(n):
        pltpu.make_async_copy(imgs[0].at[pl.ds(0, bn)], T.at[pl.ds(0, bn)], tsem.at[n]).wait()

    def load_sum(n):
        for j, lo, size, at in runs:
            if lo // bn == n:
                pltpu.make_async_copy(tins[j].at[pl.ds(at, size)], TO.at[pl.ds(lo, size)], osem.at[n]).start()

    def wait_sum(n):
        pltpu.make_async_copy(ios[0].at[pl.ds(0, bn)], TO.at[pl.ds(0, bn)], osem.at[n]).wait()

    def flush(n):
        for q, run in enumerate(out_runs):
            if run[1] // bn == n:
                flush_copy(q).start()

    def flush_copy(q):
        j, lo, size, at = out_runs[q]
        return pltpu.make_async_copy(TO.at[pl.ds(lo, size)], tos[j].at[pl.ds(at, size)], fsem.at[q])

    def when_seg(g, fn):
        for k in range(nseg):
            if nseg == 1:
                fn(k)
            else:
                pl.when((g >= starts[k]) & (g < starts[k + 1]))(functools.partial(fn, k))

    acc_src = []
    q = 0
    for k in range(nseg):
        acc_src.append(iins[q] if seg_acc[k] else None)
        q += seg_acc[k]

    def fetch(g):
        def one(k):
            rows = pl.ds((g - starts[k]) * BM, BM)
            pltpu.make_async_copy(imgs[k].at[rows], I.at[g % 4], isem.at[g % 4]).start()
            if seg_acc[k]:
                pltpu.make_async_copy(acc_src[k].at[rows], A.at[g % 4], asem.at[g % 4]).start()

        when_seg(g, one)

    def wait_img(g):
        pltpu.make_async_copy(imgs[0].at[pl.ds(0, BM)], I.at[g % 4], isem.at[g % 4]).wait()

    def open_acc(g):
        def one(k):
            if seg_acc[k]:
                pltpu.make_async_copy(acc_src[k].at[pl.ds(0, BM)], A.at[g % 4], asem.at[g % 4]).wait()
            else:
                A[g % 4] = jnp.zeros((BM, D), jnp.float32)

        when_seg(g, one)

    def put(g):
        def one(k):
            pltpu.make_async_copy(A.at[g % 4], ios[k].at[pl.ds((g - starts[k]) * BM, BM)], wsem.at[g % 4]).start()

        when_seg(g, one)

    def wait_put(g):
        pltpu.make_async_copy(A.at[g % 4], ios[0].at[pl.ds(0, BM)], wsem.at[g % 4]).wait()

    load_text(0)
    fetch(jnp.int32(0))
    for n in range(1, nth):
        load_text(n)
    if tins:
        for n in range(nth):
            load_sum(n)
    else:
        TO[...] = jnp.zeros((Q, D), jnp.float32)
    sums[...] = sin[...]

    def tile(n):
        return pl.ds(pl.multiple_of(n * bn, bn), bn)


    def s1(g, n):
        S[...] = lax.dot_general(I[g % 4], T[tile(n), :], (((1,), (1,)), ((), ())), preferred_element_type=jnp.float32)

    def s2_strip(g, n, r0, accs, z):
        rs = pl.ds(r0, STRIP)
        dot = S[rs, :]
        bias = b2
        if z is not None:
            bz = z + b2
            bias = jnp.concatenate([bz] * (STRIP // 8), axis=0)
            bias = jnp.concatenate([bias] * (bn // 128), axis=1)
        v = dot * s2_ + bias
        if diag:
            rows = g * BM + r0 + lax.broadcasted_iota(jnp.int32, (STRIP, bn), 0)
            cols = n * bn + lax.broadcasted_iota(jnp.int32, (STRIP, bn), 1)
            on = rows == cols
            v = jnp.where(on, -v, v)
        w = jnp.minimum(v, 120.0)
        e = jnp.exp2(w)
        r = 1.0 / (1.0 + e)
        c = e * r
        fix = (1.0 - r) - c
        lg = jnp.log2(r) - (v - w)
        if diag:
            c = jnp.where(on, -c, c)
        C[rs, :] = c.astype(jnp.bfloat16)
        for q, val in enumerate((lg, fix, c, c * dot)):
            for k in range(0, STRIP, 8):
                for d0 in range(0, bn, LANES):
                    accs[q] = accs[q] + val[k : k + 8, d0 : d0 + LANES]

    def s2(g, n, toks=None):
        accs = [jnp.zeros((8, LANES), jnp.float32)] * 4
        NS = BM // STRIP
        for i in range(NS):
            z = None
            if toks:
                z = toks[min(len(toks) - 1, i * len(toks) // NS)] * 0.0
            s2_strip(g, n, i * STRIP, accs, z)
        for q in range(4):
            sums[q] += accs[q]

    def s3(g, n, toks):
        s3_img(g, n, toks)
        s3_txt(g, n, toks)

    def s3_img(g, n, toks):
        for d0 in range(0, D, CHUNK):
            val = A[g % 4, :, pl.ds(d0, CHUNK)] + jnp.dot(CR[...], T[tile(n), pl.ds(d0, CHUNK)], preferred_element_type=jnp.float32)
            A[g % 4, :, pl.ds(d0, CHUNK)] = val
            toks.append(val[:8, :128])

    def s3_txt(g, n, toks):
        for d0 in range(0, D, CHUNK):
            val = TO[tile(n), pl.ds(d0, CHUNK)] + lax.dot_general(CR[...], I[g % 4, :, pl.ds(d0, CHUNK)], (((0,), (0,)), ((), ())), preferred_element_type=jnp.float32)
            TO[tile(n), pl.ds(d0, CHUNK)] = val
            toks.append(val[:8, :128])

    wait_text(0)
    wait_img(jnp.int32(0))
    fetch(jnp.int32(1))
    s1(jnp.int32(0), 0)

    def split(t):
        return t // nth, t % nth

    def unit(t, with3):
        g, h = split(t)
        gp, hp = split(t - 1)
        gq, hq = split(t - 2)

        @pl.when(h == 0)
        def _():
            wait_img(g)

            @pl.when(g >= 3)
            def _():
                wait_put(g - 3)

            @pl.when(g + 1 < G)
            def _():
                fetch(g + 1)

        if with3:
            @pl.when(hq == 0)
            def _():
                open_acc(gq)

            if nth > 2:
                @pl.when(g == 0)
                def _():
                    wait_text(h)

            if tins:
                @pl.when(gq == 0)
                def _():
                    wait_sum(hq)

        toks = []
        if with3:
            CR[...] = C[...]
            s3(gq, hq, toks)
        s2(gp, hp, toks)
        s1(g, h)
        if with3:
            @pl.when(hq == nth - 1)
            def _():
                put(gq)

    for n in range(1, min(nth, 2)):
        wait_text(n)
    unit(jnp.int32(1), False)

    def body(t, carry):
        unit(t, True)
        return carry

    NU = G * nth
    lax.fori_loop(2, NU, body, 0)
    gl = jnp.int32(G - 1)
    ga, ha = (NU - 2) // nth, (NU - 2) % nth
    if ha == 0:
        open_acc(jnp.int32(ga))
    for n in range(nth - 2):
        flush(n)
    CR[...] = C[...]
    toks = []
    s3(jnp.int32(ga), ha, toks)
    s2(gl, nth - 1, toks)
    if ha == nth - 1:
        put(jnp.int32(ga))
    else:
        flush(nth - 2)
    if nth == 1:
        open_acc(gl)
    CR[...] = C[...]
    s3_img(gl, nth - 1, [])
    put(gl)
    s3_txt(gl, nth - 1, [])
    flush(nth - 1)
    for g in range(max(0, G - 3), G):
        wait_put(jnp.int32(g))
    for q in range(len(out_runs)):
        flush_copy(q).wait()


def panel(sc, sums, imgs, iins, txts, tins, diag=False, bn=512, cuts=None):
    return panel_call(sc, sums, imgs, iins, txts, tins, diag, bn, cuts or tuple(a.shape[0] for a in txts))


def panel_call(sc, sums, imgs, iins, txts, tins, diag, bn, cuts):
    D = imgs[0].shape[1]
    cfg = (tuple(a.shape[0] // BM for a in imgs), tuple(a is not None for a in iins), tuple(a.shape[0] for a in txts), tuple(a is not None for a in tins), diag, bn, cuts)
    M, Q = sum(a.shape[0] for a in imgs), sum(a.shape[0] for a in txts)
    hbm = pl.BlockSpec(memory_space=pl.ANY)
    args = [sc, sums, *imgs, *txts, *[a for a in tins if a is not None]]
    na = len(args)
    ia = [a for a in iins if a is not None]
    args += ia
    out_shape = [jax.ShapeDtypeStruct(sums.shape, jnp.float32)]
    out_shape += [jax.ShapeDtypeStruct((c, D), jnp.float32) for c in cuts] + [jax.ShapeDtypeStruct(a.shape, jnp.float32) for a in imgs]
    alias = {}
    q = na
    for k, a in enumerate(iins):
        if a is not None:
            alias[q] = 1 + len(cuts) + k
            q += 1
    in_specs = [pl.BlockSpec(memory_space=pltpu.SMEM), pl.BlockSpec(memory_space=pltpu.VMEM)] + [hbm] * (len(args) - 2)
    out_specs = [pl.BlockSpec(memory_space=pltpu.VMEM)] + [hbm] * (len(out_shape) - 1)
    outs = pl.pallas_call(
        functools.partial(panel_body, cfg),
        out_shape=out_shape,
        in_specs=in_specs,
        out_specs=out_specs,
        input_output_aliases=alias,
        scratch_shapes=[
            pltpu.VMEM((Q, D), jnp.bfloat16),
            pltpu.VMEM((Q, D), jnp.float32),
            pltpu.VMEM((4, BM, D), jnp.bfloat16),
            pltpu.VMEM((4, BM, D), jnp.float32),
            pltpu.VMEM((BM, bn), jnp.float32),
            pltpu.VMEM((BM, bn), jnp.bfloat16),
            pltpu.VMEM((BM, bn), jnp.bfloat16),
            pltpu.SemaphoreType.DMA((Q // bn,)),
            pltpu.SemaphoreType.DMA((Q // bn,)),
            pltpu.SemaphoreType.DMA((Q // bn + len(cuts),)),
            pltpu.SemaphoreType.DMA((4,)),
            pltpu.SemaphoreType.DMA((4,)),
            pltpu.SemaphoreType.DMA((4,)),
        ],
        cost_estimate=pl.CostEstimate(flops=6 * M * Q * D, bytes_accessed=10 * M * D, transcendentals=3 * M * Q),
        compiler_params=pltpu.CompilerParams(vmem_limit_bytes=58 * 1024 * 1024),
        name="panel",
    )(*args)
    return outs[0], list(outs[1 : 1 + len(cuts)]), list(outs[1 + len(cuts) :])


def combine_body(starts, factor, base, *refs):
    refs = list(refs)
    out = refs.pop()
    g = pl.program_id(0)
    out[...] = base[...]
    for ref, (lo, hi) in zip(refs, starts):
        @pl.when((g >= lo) & (g < hi))
        def _():
            out[...] += ref[...]

    out[...] *= factor[0]


def combine_call(factor, base, items):
    rows, D = base.shape
    br = 256
    starts, specs = [], []
    for lo, piece in items:
        lo, n = lo // br, piece.shape[0] // br
        starts.append((lo, lo + n))
        specs.append(pl.BlockSpec((br, D), functools.partial(lambda lo, n, g: (jnp.clip(g - lo, 0, n - 1), 0), lo, n)))
    row = pl.BlockSpec((br, D), lambda g: (g, 0))
    return pl.pallas_call(
        functools.partial(combine_body, tuple(starts)),
        grid=(rows // br,),
        out_shape=jax.ShapeDtypeStruct(base.shape, jnp.float32),
        in_specs=[pl.BlockSpec(memory_space=pltpu.SMEM), row, *specs],
        out_specs=row,
        compiler_params=pltpu.CompilerParams(vmem_limit_bytes=32 * 1024 * 1024),
        cost_estimate=pl.CostEstimate(flops=rows * D * 64, bytes_accessed=16 * rows * D, transcendentals=0),
        name="combine",
    )(factor.reshape(1), base, *[piece for _, piece in items])


def add_rows_body(starts, factor, base, *refs):
    refs = list(refs)
    out = refs.pop()
    g = pl.program_id(0)
    for ref, (lo, hi) in zip(refs, starts):
        @pl.when((g >= lo) & (g < hi))
        def _():
            out[...] = base[...] + ref[...] * factor[0]


def add_rows(factor, base, row, pieces):
    D = base.shape[1]
    br = 128
    first = row // br
    starts, specs, lo = [], [], 0
    for piece in pieces:
        n = piece.shape[0] // br
        starts.append((lo, lo + n))
        specs.append(pl.BlockSpec((br, D), functools.partial(lambda lo, n, g: (jnp.clip(g - lo, 0, n - 1), 0), lo, n)))
        lo += n
    late = pl.BlockSpec((br, D), lambda g: (first + g, 0))
    return pl.pallas_call(
        functools.partial(add_rows_body, tuple(starts)),
        grid=(lo,),
        out_shape=jax.ShapeDtypeStruct(base.shape, jnp.float32),
        in_specs=[pl.BlockSpec(memory_space=pltpu.SMEM), late, *specs],
        out_specs=late,
        input_output_aliases={1: 0},
        compiler_params=pltpu.CompilerParams(vmem_limit_bytes=32 * 1024 * 1024),
        cost_estimate=pl.CostEstimate(flops=lo * br * D * 64, bytes_accessed=12 * lo * br * D, transcendentals=0),
        name="add_rows",
    )(factor.reshape(1), base, *pieces)


def solution(mesh):
    axis = mesh.axis_names[0]
    n_dev = mesh.shape[axis]

    def swap(a, mask):
        return lax.ppermute(a, axis, [(i, i ^ mask) for i in range(n_dev)])

    CORE, X, Y, Z = 1, 2, 4, 8

    def step(img, txt, log_temp, logit_bias):
        rows = img.shape[0]
        n_total = rows * n_dev
        scale = jnp.exp(log_temp[0])
        sc = jnp.stack([scale * LOG2E, logit_bias[0] * LOG2E])
        sums = jnp.zeros((4, 8, LANES), jnp.float32)
        ha, hb = slice(0, rows // 2), slice(rows // 2, rows)
        third = rows // 3

        img_c = swap(img, CORE)
        x0, x1, x2 = (swap(img[k * third : (k + 1) * third], X) for k in range(3))
        xc0, xc1, xc2 = (swap(a, CORE) for a in (x0, x1, x2))
        ya = swap(txt[ha], Y)
        zb = swap(txt[hb], Z)
        yza = swap(ya, Z)
        yzb = swap(zb, Y)
        yb = swap(txt[hb], Y)
        za = swap(txt[ha], Z)

        OC, X0, X1, X2 = [img, img_c], [x0, xc0], [x1, xc1], [x2, xc2]
        N2 = [None, None]

        def reduce_x(acc, acc_c):
            return swap(acc + swap(acc_c, CORE), X)

        sums, own, oc = panel(sc, sums, OC, N2, [txt], [None], diag=True)
        sums, own, ax = panel(sc, sums, X0 + X1, N2 + N2, [txt], own)
        sums, p_yz, accs = panel(sc, sums, OC + X0 + X1 + X2, oc + ax + N2, [yza, yzb], N2)
        ry, rz = swap(p_yz[0], Z), swap(p_yz[1], Y)
        sums, p_zayb, accs = panel(sc, sums, OC + X0 + X1 + X2, accs, [za, yb], N2)
        ao, ac, a0, ac0, a1, ac1, a2, ac2 = accs
        fz, fy = swap(p_zayb[0], Z), swap(p_zayb[1], Y)
        sums, p_yazb, (a0, ac0, ac1) = panel(sc, sums, [x0, xc0, xc1], [a0, ac0, ac1], [ya, zb], [ry, rz])
        gx0 = reduce_x(a0, ac0)
        sums, p_yazb, (a1, ac2) = panel(sc, sums, [x1, xc2], [a1, ac2], [ya, zb], p_yazb)
        gx1 = reduce_x(a1, ac1)
        sums, p_yazb, (ao, ac, a2) = panel(sc, sums, OC + [x2], [ao, ac, a2], [ya, zb], p_yazb, cuts=(512, 256, 256, 512))
        gy0, gy1 = swap(p_yazb[0], Y), swap(p_yazb[1], Y)
        gz0, gz1 = swap(p_yazb[3], Z), swap(p_yazb[2], Z)
        gc = swap(ac, CORE)
        sums, own, (a2, ac2) = panel(sc, sums, X2, [a2, ac2], [txt], own)
        gx2 = reduce_x(a2, ac2)

        factor = scale / n_total
        txt_pre = combine_call(jnp.ones((), jnp.float32), own[0], [(0, fz), (rows // 2, fy)])
        img_pre = combine_call(factor, ao, [(0, gc), (0, gx0), (third, gx1)])
        txt_most = combine_call(factor, txt_pre, [(0, gy0), (2 * third, gz0)])
        txt_grad = add_rows(factor, txt_most, third, [gy1, gz1])
        img_grad = add_rows(factor, img_pre, 2 * third, [gx2])
        tot = jnp.sum(sums, axis=(1, 2))
        tot = tot + swap(tot, CORE)
        tot = tot + swap(tot, X)
        tot = (tot + swap(tot, Y)) + (swap(tot, Z) + swap(tot, Y | Z))
        loss = -(tot[0:1] * LN2 + tot[1:2]) / n_total
        return loss, img_grad, txt_grad, tot[3:4] * factor, tot[2:3] / n_total

    split = P(axis, None)
    return jax.shard_map(step, mesh=mesh, in_specs=(split, split, P(None), P(None)), out_specs=(P(None), split, split, P(None), P(None)), check_vma=False)
```

```python
import functools
import jax
import jax.numpy as jnp
from jax import lax
from jax.experimental import pallas as pl
from jax.experimental.pallas import tpu as pltpu
from jax.sharding import PartitionSpec as P

LOG2E = 1.4426950408889634
LN2 = 0.6931471805599453
BM = 512
STRIP = 32
CHUNK = 512
LANES = 256


def panel_body(cfg, *refs):
    seg_chunks, seg_acc, pieces, tin_flags, diag, bn, cuts = cfg
    refs = list(refs)
    take = lambda n: [refs.pop(0) for _ in range(n)]
    nseg, npc = len(seg_chunks), len(pieces)
    (sc,) = take(1)
    (sin,) = take(1)
    imgs, txts = take(nseg), take(npc)
    tins = take(sum(tin_flags))
    iins = take(sum(seg_acc))
    zero = None if all(seg_acc) else take(1)[0]
    (sums,) = take(1)
    tos, ios = take(len(cuts)), take(nseg)
    T, TO, I, A, S, C, CR, tsem, osem, fsem, isem, asem, wsem = refs
    starts = [sum(seg_chunks[:k]) for k in range(nseg + 1)]
    G = starts[-1]
    Q = sum(pieces)
    D = T.shape[1]
    nth = Q // bn
    s2_, b2 = sc[0], sc[1]

    def cut_runs(sizes):
        runs, at = [], 0
        for j, size in enumerate(sizes):
            lo = at
            while lo < at + size:
                hi = min((lo // bn + 1) * bn, at + size)
                runs.append((j, lo, hi - lo, lo - at))
                lo = hi
            at += size
        return runs

    runs, out_runs = cut_runs(pieces), cut_runs(cuts)

    def load_text(n):
        for j, lo, size, at in runs:
            if lo // bn == n:
                pltpu.make_async_copy(txts[j].at[pl.ds(at, size)], T.at[pl.ds(lo, size)], tsem.at[n]).start()

    def wait_text(n):
        pltpu.make_async_copy(imgs[0].at[pl.ds(0, bn)], T.at[pl.ds(0, bn)], tsem.at[n]).wait()

    def load_sum(n):
        for j, lo, size, at in runs:
            if lo // bn == n:
                pltpu.make_async_copy(tins[j].at[pl.ds(at, size)], TO.at[pl.ds(lo, size)], osem.at[n]).start()

    def wait_sum(n):
        pltpu.make_async_copy(ios[0].at[pl.ds(0, bn)], TO.at[pl.ds(0, bn)], osem.at[n]).wait()

    def flush(n):
        for q, run in enumerate(out_runs):
            if run[1] // bn == n:
                flush_copy(q).start()

    def flush_copy(q):
        j, lo, size, at = out_runs[q]
        return pltpu.make_async_copy(TO.at[pl.ds(lo, size)], tos[j].at[pl.ds(at, size)], fsem.at[q])

    def when_seg(g, fn):
        for k in range(nseg):
            if nseg == 1:
                fn(k)
            else:
                pl.when((g >= starts[k]) & (g < starts[k + 1]))(functools.partial(fn, k))

    acc_src = []
    q = 0
    for k in range(nseg):
        acc_src.append(iins[q] if seg_acc[k] else None)
        q += seg_acc[k]

    def fetch(g):
        def one(k):
            rows = pl.ds((g - starts[k]) * BM, BM)
            pltpu.make_async_copy(imgs[k].at[rows], I.at[g % 4], isem.at[g % 4]).start()
            src = acc_src[k].at[rows] if seg_acc[k] else zero
            pltpu.make_async_copy(src, A.at[g % 4], asem.at[g % 4]).start()

        when_seg(g, one)

    def wait_img(g):
        pltpu.make_async_copy(imgs[0].at[pl.ds(0, BM)], I.at[g % 4], isem.at[g % 4]).wait()

    def open_acc(g):
        pltpu.make_async_copy(ios[0].at[pl.ds(0, BM)], A.at[g % 4], asem.at[g % 4]).wait()

    def put(g):
        def one(k):
            pltpu.make_async_copy(A.at[g % 4], ios[k].at[pl.ds((g - starts[k]) * BM, BM)], wsem.at[g % 4]).start()

        when_seg(g, one)

    def wait_put(g):
        pltpu.make_async_copy(A.at[g % 4], ios[0].at[pl.ds(0, BM)], wsem.at[g % 4]).wait()

    load_text(0)
    fetch(jnp.int32(0))
    for n in range(1, nth):
        load_text(n)
    if tins:
        for n in range(nth):
            load_sum(n)
    else:
        TO[...] = jnp.zeros((Q, D), jnp.float32)
    sums[...] = sin[...]

    def tile(n):
        return pl.ds(pl.multiple_of(n * bn, bn), bn)


    def s1(g, n):
        S[...] = lax.dot_general(I[g % 4], T[tile(n), :], (((1,), (1,)), ((), ())), preferred_element_type=jnp.float32)

    def s2_strip(g, n, r0, accs, z):
        rs = pl.ds(r0, STRIP)
        dot = S[rs, :]
        bias = b2
        if z is not None:
            bz = z + b2
            bias = jnp.concatenate([bz] * (STRIP // 8), axis=0)
            bias = jnp.concatenate([bias] * (bn // 128), axis=1)
        v = dot * s2_ + bias
        if diag:
            rows = g * BM + r0 + lax.broadcasted_iota(jnp.int32, (STRIP, bn), 0)
            cols = n * bn + lax.broadcasted_iota(jnp.int32, (STRIP, bn), 1)
            on = rows == cols
            v = jnp.where(on, -v, v)
        w = jnp.minimum(v, 120.0)
        e = jnp.exp2(w)
        r = 1.0 / (1.0 + e)
        c = e * r
        fix = (1.0 - r) - c
        lg = jnp.log2(r) - (v - w)
        if diag:
            c = jnp.where(on, -c, c)
        C[rs, :] = c.astype(jnp.bfloat16)
        for q, val in enumerate((lg, fix, c, c * dot)):
            for k in range(0, STRIP, 8):
                for d0 in range(0, bn, LANES):
                    accs[q] = accs[q] + val[k : k + 8, d0 : d0 + LANES]

    def s2(g, n, toks=None):
        accs = [jnp.zeros((8, LANES), jnp.float32)] * 4
        NS = BM // STRIP
        for i in range(NS):
            z = None
            if toks:
                z = toks[min(len(toks) - 1, i * len(toks) // NS)] * 0.0
            s2_strip(g, n, i * STRIP, accs, z)
        for q in range(4):
            sums[q] += accs[q]

    def s3(g, n, toks):
        s3_img(g, n, toks)
        s3_txt(g, n, toks)

    def s3_img(g, n, toks):
        for d0 in range(0, D, CHUNK):
            val = A[g % 4, :, pl.ds(d0, CHUNK)] + jnp.dot(CR[...], T[tile(n), pl.ds(d0, CHUNK)], preferred_element_type=jnp.float32)
            A[g % 4, :, pl.ds(d0, CHUNK)] = val
            toks.append(val[:8, :128])

    def s3_txt(g, n, toks):
        for d0 in range(0, D, CHUNK):
            val = TO[tile(n), pl.ds(d0, CHUNK)] + lax.dot_general(CR[...], I[g % 4, :, pl.ds(d0, CHUNK)], (((0,), (0,)), ((), ())), preferred_element_type=jnp.float32)
            TO[tile(n), pl.ds(d0, CHUNK)] = val
            toks.append(val[:8, :128])

    wait_text(0)
    wait_img(jnp.int32(0))
    fetch(jnp.int32(1))
    s1(jnp.int32(0), 0)

    def split(t):
        return t // nth, t % nth

    def unit(t, with3):
        g, h = split(t)
        gp, hp = split(t - 1)
        gq, hq = split(t - 2)

        @pl.when(h == 0)
        def _():
            wait_img(g)

            @pl.when(g >= 3)
            def _():
                wait_put(g - 3)

            @pl.when(g + 1 < G)
            def _():
                fetch(g + 1)

        if with3:
            @pl.when(hq == 0)
            def _():
                open_acc(gq)

            if nth > 2:
                @pl.when(g == 0)
                def _():
                    wait_text(h)

            if tins:
                @pl.when(gq == 0)
                def _():
                    wait_sum(hq)

        toks = []
        if with3:
            CR[...] = C[...]
            s3(gq, hq, toks)
        s2(gp, hp, toks)
        s1(g, h)
        if with3:
            @pl.when(hq == nth - 1)
            def _():
                put(gq)

    for n in range(1, min(nth, 2)):
        wait_text(n)
    unit(jnp.int32(1), False)

    def body(t, carry):
        unit(t, True)
        return carry

    NU = G * nth
    lax.fori_loop(2, NU, body, 0)
    gl = jnp.int32(G - 1)
    ga, ha = (NU - 2) // nth, (NU - 2) % nth
    if ha == 0:
        open_acc(jnp.int32(ga))
    for n in range(nth - 2):
        flush(n)
    CR[...] = C[...]
    toks = []
    s3(jnp.int32(ga), ha, toks)
    s2(gl, nth - 1, toks)
    if ha == nth - 1:
        put(jnp.int32(ga))
    else:
        flush(nth - 2)
    if nth == 1:
        open_acc(gl)
    CR[...] = C[...]
    s3_img(gl, nth - 1, [])
    put(gl)
    s3_txt(gl, nth - 1, [])
    flush(nth - 1)
    for g in range(max(0, G - 3), G):
        wait_put(jnp.int32(g))
    for q in range(len(out_runs)):
        flush_copy(q).wait()


def panel(sc, sums, imgs, iins, txts, tins, diag=False, bn=512, cuts=None):
    return panel_call(sc, sums, imgs, iins, txts, tins, diag, bn, cuts or tuple(a.shape[0] for a in txts))


def panel_call(sc, sums, imgs, iins, txts, tins, diag, bn, cuts):
    D = imgs[0].shape[1]
    cfg = (tuple(a.shape[0] // BM for a in imgs), tuple(a is not None for a in iins), tuple(a.shape[0] for a in txts), tuple(a is not None for a in tins), diag, bn, cuts)
    M, Q = sum(a.shape[0] for a in imgs), sum(a.shape[0] for a in txts)
    hbm = pl.BlockSpec(memory_space=pl.ANY)
    args = [sc, sums, *imgs, *txts, *[a for a in tins if a is not None]]
    na = len(args)
    ia = [a for a in iins if a is not None]
    args += ia
    if len(ia) < len(iins):
        args.append(jnp.zeros((BM, D), jnp.float32))
    out_shape = [jax.ShapeDtypeStruct(sums.shape, jnp.float32)]
    out_shape += [jax.ShapeDtypeStruct((c, D), jnp.float32) for c in cuts] + [jax.ShapeDtypeStruct(a.shape, jnp.float32) for a in imgs]
    alias = {}
    q = na
    for k, a in enumerate(iins):
        if a is not None:
            alias[q] = 1 + len(cuts) + k
            q += 1
    in_specs = [pl.BlockSpec(memory_space=pltpu.SMEM), pl.BlockSpec(memory_space=pltpu.VMEM)] + [hbm] * (len(args) - 2)
    out_specs = [pl.BlockSpec(memory_space=pltpu.VMEM)] + [hbm] * (len(out_shape) - 1)
    outs = pl.pallas_call(
        functools.partial(panel_body, cfg),
        out_shape=out_shape,
        in_specs=in_specs,
        out_specs=out_specs,
        input_output_aliases=alias,
        scratch_shapes=[
            pltpu.VMEM((Q, D), jnp.bfloat16),
            pltpu.VMEM((Q, D), jnp.float32),
            pltpu.VMEM((4, BM, D), jnp.bfloat16),
            pltpu.VMEM((4, BM, D), jnp.float32),
            pltpu.VMEM((BM, bn), jnp.float32),
            pltpu.VMEM((BM, bn), jnp.bfloat16),
            pltpu.VMEM((BM, bn), jnp.bfloat16),
            pltpu.SemaphoreType.DMA((Q // bn,)),
            pltpu.SemaphoreType.DMA((Q // bn,)),
            pltpu.SemaphoreType.DMA((Q // bn + len(cuts),)),
            pltpu.SemaphoreType.DMA((4,)),
            pltpu.SemaphoreType.DMA((4,)),
            pltpu.SemaphoreType.DMA((4,)),
        ],
        cost_estimate=pl.CostEstimate(flops=6 * M * Q * D, bytes_accessed=10 * M * D, transcendentals=3 * M * Q),
        compiler_params=pltpu.CompilerParams(vmem_limit_bytes=58 * 1024 * 1024),
        name="panel",
    )(*args)
    return outs[0], list(outs[1 : 1 + len(cuts)]), list(outs[1 + len(cuts) :])


def combine_body(starts, factor, base, *refs):
    refs = list(refs)
    out = refs.pop()
    g = pl.program_id(0)
    out[...] = base[...]
    for ref, (lo, hi) in zip(refs, starts):
        @pl.when((g >= lo) & (g < hi))
        def _():
            out[...] += ref[...]

    out[...] *= factor[0]


def combine_call(factor, base, items):
    rows, D = base.shape
    br = 256
    starts, specs = [], []
    for lo, piece in items:
        lo, n = lo // br, piece.shape[0] // br
        starts.append((lo, lo + n))
        specs.append(pl.BlockSpec((br, D), functools.partial(lambda lo, n, g: (jnp.clip(g - lo, 0, n - 1), 0), lo, n)))
    row = pl.BlockSpec((br, D), lambda g: (g, 0))
    return pl.pallas_call(
        functools.partial(combine_body, tuple(starts)),
        grid=(rows // br,),
        out_shape=jax.ShapeDtypeStruct(base.shape, jnp.float32),
        in_specs=[pl.BlockSpec(memory_space=pltpu.SMEM), row, *specs],
        out_specs=row,
        compiler_params=pltpu.CompilerParams(vmem_limit_bytes=32 * 1024 * 1024),
        cost_estimate=pl.CostEstimate(flops=rows * D * 64, bytes_accessed=16 * rows * D, transcendentals=0),
        name="combine",
    )(factor.reshape(1), base, *[piece for _, piece in items])


def add_rows_body(starts, factor, base, *refs):
    refs = list(refs)
    out = refs.pop()
    g = pl.program_id(0)
    for ref, (lo, hi) in zip(refs, starts):
        @pl.when((g >= lo) & (g < hi))
        def _():
            out[...] = base[...] + ref[...] * factor[0]


def add_rows(factor, base, row, pieces):
    D = base.shape[1]
    br = 128
    first = row // br
    starts, specs, lo = [], [], 0
    for piece in pieces:
        n = piece.shape[0] // br
        starts.append((lo, lo + n))
        specs.append(pl.BlockSpec((br, D), functools.partial(lambda lo, n, g: (jnp.clip(g - lo, 0, n - 1), 0), lo, n)))
        lo += n
    late = pl.BlockSpec((br, D), lambda g: (first + g, 0))
    return pl.pallas_call(
        functools.partial(add_rows_body, tuple(starts)),
        grid=(lo,),
        out_shape=jax.ShapeDtypeStruct(base.shape, jnp.float32),
        in_specs=[pl.BlockSpec(memory_space=pltpu.SMEM), late, *specs],
        out_specs=late,
        input_output_aliases={1: 0},
        compiler_params=pltpu.CompilerParams(vmem_limit_bytes=32 * 1024 * 1024),
        cost_estimate=pl.CostEstimate(flops=lo * br * D * 64, bytes_accessed=12 * lo * br * D, transcendentals=0),
        name="add_rows",
    )(factor.reshape(1), base, *pieces)


def solution(mesh):
    axis = mesh.axis_names[0]
    n_dev = mesh.shape[axis]

    def swap(a, mask):
        return lax.ppermute(a, axis, [(i, i ^ mask) for i in range(n_dev)])

    CORE, X, Y, Z = 1, 2, 4, 8

    def step(img, txt, log_temp, logit_bias):
        rows = img.shape[0]
        n_total = rows * n_dev
        scale = jnp.exp(log_temp[0])
        sc = jnp.stack([scale * LOG2E, logit_bias[0] * LOG2E])
        sums = jnp.zeros((4, 8, LANES), jnp.float32)
        ha, hb = slice(0, rows // 2), slice(rows // 2, rows)
        third = rows // 3

        img_c = swap(img, CORE)
        x0, x1, x2 = (swap(img[k * third : (k + 1) * third], X) for k in range(3))
        xc0, xc1, xc2 = (swap(a, CORE) for a in (x0, x1, x2))
        ya = swap(txt[ha], Y)
        zb = swap(txt[hb], Z)
        yza = swap(ya, Z)
        yzb = swap(zb, Y)
        yb = swap(txt[hb], Y)
        za = swap(txt[ha], Z)

        OC, X0, X1, X2 = [img, img_c], [x0, xc0], [x1, xc1], [x2, xc2]
        N2 = [None, None]

        def reduce_x(acc, acc_c):
            return swap(acc + swap(acc_c, CORE), X)

        sums, own, oc = panel(sc, sums, OC, N2, [txt], [None], diag=True)
        sums, own, ax = panel(sc, sums, X0 + X1, N2 + N2, [txt], own)
        sums, p_yz, accs = panel(sc, sums, OC + X0 + X1 + X2, oc + ax + N2, [yza, yzb], N2)
        ry, rz = swap(p_yz[0], Z), swap(p_yz[1], Y)
        sums, p_zayb, accs = panel(sc, sums, OC + X0 + X1 + X2, accs, [za, yb], N2)
        ao, ac, a0, ac0, a1, ac1, a2, ac2 = accs
        fz, fy = swap(p_zayb[0], Z), swap(p_zayb[1], Y)
        sums, p_yazb, (a0, ac0, ac1) = panel(sc, sums, [x0, xc0, xc1], [a0, ac0, ac1], [ya, zb], [ry, rz])
        gx0 = reduce_x(a0, ac0)
        sums, p_yazb, (a1, ac2) = panel(sc, sums, [x1, xc2], [a1, ac2], [ya, zb], p_yazb)
        gx1 = reduce_x(a1, ac1)
        sums, p_yazb, (ao, ac, a2) = panel(sc, sums, OC + [x2], [ao, ac, a2], [ya, zb], p_yazb, cuts=(512, 256, 256, 512))
        gy0, gy1 = swap(p_yazb[0], Y), swap(p_yazb[1], Y)
        gz0, gz1 = swap(p_yazb[3], Z), swap(p_yazb[2], Z)
        gc = swap(ac, CORE)
        sums, own, (a2, ac2) = panel(sc, sums, X2, [a2, ac2], [txt], own)
        gx2 = reduce_x(a2, ac2)

        factor = scale / n_total
        txt_pre = combine_call(jnp.ones((), jnp.float32), own[0], [(0, fz), (rows // 2, fy)])
        img_pre = combine_call(factor, ao, [(0, gc), (0, gx0), (third, gx1)])
        txt_most = combine_call(factor, txt_pre, [(0, gy0), (2 * third, gz0)])
        txt_grad = add_rows(factor, txt_most, third, [gy1, gz1])
        img_grad = add_rows(factor, img_pre, 2 * third, [gx2])
        tot = jnp.sum(sums, axis=(1, 2))
        tot = tot + swap(tot, CORE)
        tot = tot + swap(tot, X)
        tot = (tot + swap(tot, Y)) + (swap(tot, Z) + swap(tot, Y | Z))
        loss = -(tot[0:1] * LN2 + tot[1:2]) / n_total
        return loss, img_grad, txt_grad, tot[3:4] * factor, tot[2:3] / n_total

    split = P(axis, None)
    return jax.shard_map(step, mesh=mesh, in_specs=(split, split, P(None), P(None)), out_specs=(P(None), split, split, P(None), P(None)), check_vma=False)
```
